256 devices in a mesh: node: 128 (over x_lo, z, y, core), blk: 2 (over x_hi).
Axes of the slice: x: 4 (x_hi: 2, x_lo: 2; x = x_hi * 2 + x_lo), y: 4, z: 8, core: 2. Of those that a mesh axis runs over, the one named last changes fastest.
Arguments:
- params: bfloat16 [128, 128, 14336], P('node', 'blk'), may hold values from -40 to 40
- weights: int32 [128], P('node'), may hold values from 1 to 8
Outputs:
- debiased: float32 [128, 128, 14336], P('node', 'blk')
- average: float32 [128, 14336], P('blk', 'node')
- spread: float32 [128], P('node')
The draws below stay inside these ranges and needn't reach their ends.
All inputs are finite; a program needn't handle non-finite values.
Results may differ from the reference program's by a relative error of at most 0.0003.
Values may be sent and summed in bfloat16 or wider, within the bound.
No kernel may reach another device: no remote copies, remote signals or barrier semaphores. Data moves between devices by JAX's collectives and lax.ppermute only.
A program may use at most 64 MiB of HBM per device.

```python
import jax
import jax.numpy as jnp

FF = 14336
ROUNDS = 3
ROWS = 128
NODES = 128


def draw_params(key, part):
    keys = jax.random.split(jax.random.fold_in(key, 11), 3)
    index = jnp.arange(NODES, dtype=jnp.float32)
    node_scale = (1.0 + 2.0 * index / max(NODES - 1, 1)) * jax.random.uniform(keys[1], (NODES,), minval=0.8, maxval=1.2)
    base = jax.random.normal(keys[0], (NODES, ROWS, FF))
    row_scale = jnp.exp(jax.random.uniform(keys[2], (ROWS,), minval=0.0, maxval=jnp.log(3.0)))
    values = base * node_scale[:, None, None] * row_scale[None, :, None]
    return jnp.clip(values, -40.0, 40.0).astype(jnp.bfloat16)


def touch_ends(entries, key, least, largest):
    extent = entries.shape
    spot = [jax.random.randint(jax.random.fold_in(key, axis), (), 0, extent[axis]) for axis in range(len(extent))]
    entries = entries.at[tuple(spot)].set(least)
    longest = extent.index(max(extent))
    spot[longest] = (spot[longest] + 1) % extent[longest]
    return entries.at[tuple(spot)].set(largest)


def setup_inputs(seed: int = 0) -> dict:
    streams_of = jax.random.split(jax.random.key(seed), 3)
    return {
        "params": draw_params(jax.random.fold_in(streams_of[2], 71), 0),
        "weights": touch_ends(jax.random.randint(streams_of[1], (NODES,), 1, 9), jax.random.fold_in(streams_of[1], 1), 1, 8).astype(jnp.int32),
    }


def reference(params, weights):
    scale0 = weights.astype(jnp.float32)
    value = scale0[:, None, None] * params.astype(jnp.float32)
    scale = scale0
    levels = NODES.bit_length() - 1
    for step in range(ROUNDS):
        hop = 1 << (step % levels)
        value = 0.5 * value + 0.5 * jnp.roll(value, hop, 0)
        scale = 0.5 * scale + 0.5 * jnp.roll(scale, hop, 0)
    debiased = value / scale[:, None, None]
    numer = jnp.sum(scale0[:, None, None] * params.astype(jnp.float32), axis=0)
    average = numer / jnp.sum(scale0)
    spread = jnp.sum((debiased - average[None]) ** 2, axis=(1, 2)) / (ROWS * FF)
    return debiased, average, spread
```

```python
import jax
import jax.numpy as jnp
from jax import lax
from jax.experimental import pallas as pl
from jax.experimental.pallas import tpu as pltpu
from jax.sharding import Mesh
from jax.sharding import PartitionSpec as P

NODE = ("xl", "z", "y", "core")
RING = ("y", "core")
BLOCKS = ("xl", "z")
LANES = 128
F32 = jnp.float32


def to_all(value, axes):
    return lax.all_to_all(value, axes, 0, 0, tiled=True)


def column(ref, k):
    return ref[k, :, 0:1].astype(F32)


def block_sums_body(a_ref, b_ref, w_ref, out_ref):
    step = pl.program_id(0)
    count, nodes = out_ref.shape[0], a_ref.shape[0]
    width = a_ref.shape[2] // count
    w = [column(w_ref, k) for k in range(nodes)]
    total = sum(w[1:], w[0])

    def fill(ref):
        for q in range(count):
            at = slice(q * width, (q + 1) * width)
            acc = w[0] * ref[0, :, at].astype(F32)
            for k in range(1, nodes):
                acc = acc + w[k] * ref[k, :, at].astype(F32)
            out_ref[q, :, :width] = acc
            out_ref[q, :, width:] = jnp.broadcast_to(total, (acc.shape[0], LANES))

    half = pl.num_programs(0) // 2

    @pl.when(step < half)
    def _():
        fill(a_ref)

    @pl.when(step >= half)
    def _():
        fill(b_ref)


def block_sums(a, b, width, blocks):
    nodes, rows, cols = b.shape
    count = 4
    half = blocks // count // 2
    return pl.pallas_call(
        block_sums_body,
        grid=(2 * half,),
        in_specs=[
            pl.BlockSpec((nodes, rows, count * width), lambda s: (0, 0, jnp.minimum(s, half - 1))),
            pl.BlockSpec((nodes, rows, count * width), lambda s: (0, 0, jnp.maximum(s - half, 0))),
            pl.BlockSpec((nodes, rows, LANES), lambda s: (0, 0, cols // LANES)),
        ],
        out_specs=pl.BlockSpec((count, rows, width + LANES), lambda s: (s, 0, 0)),
        out_shape=jax.ShapeDtypeStruct((blocks, rows, width + LANES), F32),
        name="block_sums",
    )(a, b, a)


def weighted(ref, w, k):
    return w[k] * ref[k].astype(F32)


def chip_sums_body(own_ref, prev_ref, w_ref, v_ref, out_ref):
    nodes = own_ref.shape[0]
    w = [column(w_ref, k) for k in range(nodes)]
    v = [column(v_ref, k) for k in range(nodes - 1)]
    chips = nodes // 2
    after = [None] * chips
    for y in range(chips - 1, 0, -1):
        pair = weighted(prev_ref, v, 2 * y - 1) + weighted(prev_ref, v, 2 * y)
        after[y - 1] = pair if after[y] is None else after[y] + pair
    before = None
    for y in range(chips):
        parts = [part for part in (before, after[y]) if part is not None]
        out_ref[y] = sum(parts[1:], parts[0])
        if y < chips - 1:
            pair = weighted(own_ref, w, 2 * y) + weighted(own_ref, w, 2 * y + 1)
            before = pair if before is None else before + pair


def chip_sums(own, prev, w_from, v_from, cols):
    nodes, rows = own.shape[:2]
    width = cols // 4
    return pl.pallas_call(
        chip_sums_body,
        grid=(4,),
        in_specs=[
            pl.BlockSpec((nodes, rows, width), lambda s: (0, 0, s)),
            pl.BlockSpec((nodes - 1, rows, width), lambda s: (0, 0, s)),
            pl.BlockSpec((nodes, rows, LANES), lambda s: (0, 0, cols // LANES)),
            pl.BlockSpec((nodes - 1, rows, LANES), lambda s: (0, 0, cols // LANES)),
        ],
        out_specs=pl.BlockSpec((nodes // 2, rows, width), lambda s: (0, 0, s)),
        out_shape=jax.ShapeDtypeStruct((nodes // 2, rows, cols), F32),
        name="chip_sums",
    )(own, prev, w_from, v_from)


def deviations_body(own_ref, prev_ref, w_ref, v_ref, average_ref, out_ref):
    nodes = own_ref.shape[0]
    w = [column(w_ref, k) for k in range(nodes)]
    v = [column(v_ref, k) for k in range(nodes - 1)]
    average = jnp.concatenate([average_ref[q] for q in range(average_ref.shape[0])], axis=1)
    after, weight_after = [None] * nodes, [None] * nodes
    for c in range(nodes - 1, 0, -1):
        term = weighted(prev_ref, v, c - 1)
        after[c - 1] = term if after[c] is None else after[c] + term
        weight_after[c - 1] = v[c - 1] if after[c] is None else weight_after[c] + v[c - 1]
    before, weight = None, None

    @pl.when(pl.program_id(0) == 0)
    def _():
        out_ref[...] = jnp.zeros(out_ref.shape, F32)

    for c in range(nodes):
        term = weighted(own_ref, w, c)
        before = term if before is None else before + term
        weight = w[c] if weight is None else weight + w[c]
        value, scale = before, weight
        if after[c] is not None:
            value, scale = value + after[c], scale + weight_after[c]
        gap = value * (1.0 / scale) - average
        square = gap * gap
        acc = square[:, :LANES]
        for t in range(1, square.shape[1] // LANES):
            acc = acc + square[:, t * LANES : (t + 1) * LANES]
        out_ref[c] += acc


def deviations(own, prev, w_from, v_from, average, first, cols):
    nodes, rows = own.shape[:2]
    piece = average.shape[2]
    count = 2
    width = count * piece
    return pl.pallas_call(
        deviations_body,
        grid=(cols // width,),
        in_specs=[
            pl.BlockSpec((nodes, rows, width), lambda s: (0, 0, s)),
            pl.BlockSpec((nodes - 1, rows, width), lambda s: (0, 0, s)),
            pl.BlockSpec((nodes, rows, LANES), lambda s: (0, 0, cols // LANES)),
            pl.BlockSpec((nodes - 1, rows, LANES), lambda s: (0, 0, cols // LANES)),
            pl.BlockSpec((count, rows, piece), lambda s: (first // count + s, 0, 0)),
        ],
        out_specs=pl.BlockSpec((nodes, rows, LANES), lambda s: (0, 0, 0)),
        out_shape=jax.ShapeDtypeStruct((nodes, rows, LANES), F32),
        name="deviations",
    )(own, prev, w_from, v_from, average)


def debias_body(at_ref, p_ref, o_ref, same_ref, swap_ref, w_ref, v_ref, *rest):
    out_ref = rest[-1]
    c = at_ref[0]
    core = c % 2
    nodes, rows = w_ref.shape[:2]
    w = [column(w_ref, k) for k in range(nodes)]
    v = [None] + [column(v_ref, k) for k in range(nodes - 1)]
    scale = own = w[0]
    other = w[0]
    for k in range(1, nodes):
        scale = scale + jnp.where(k <= c, w[k], v[k])
        own = jnp.where(k == c, w[k], own)
        if k % 2:
            other = jnp.where(k == c + 1, v[k], other)
        else:
            other = jnp.where(k == c - 1, w[k], other)
    inverse = 1.0 / scale
    own, other = own * inverse, other * inverse
    same, swap = same_ref[0] * inverse, swap_ref[0] * inverse
    first = jnp.where(core == 0, same, swap)
    second = jnp.where(core == 0, swap, same)
    for at, total in ((slice(0, rows), first), (slice(rows, 2 * rows), second)):
        out_ref[at] = total + own * p_ref[at].astype(F32) + other * o_ref[at].astype(F32)


def debias(at, p, o, same, swap, w_from, v_from, chunk, cols, so_far):
    rows = same.shape[1]
    nodes = w_from.shape[0]
    split = 2
    width = cols // split
    wide = lambda y, s, at: (y, chunk * split + s)
    in_specs = [
        pl.BlockSpec((2 * rows, width), wide),
        pl.BlockSpec((2 * rows, width), wide),
        pl.BlockSpec((1, rows, width), lambda y, s, at: (y, 0, s)),
        pl.BlockSpec((1, rows, width), lambda y, s, at: (y, 0, s)),
        pl.BlockSpec((nodes, rows, LANES), lambda y, s, at: (0, 0, cols // LANES)),
        pl.BlockSpec((nodes - 1, rows, LANES), lambda y, s, at: (0, 0, cols // LANES)),
    ]
    operands = [at, p, o, same, swap, w_from, v_from]
    aliases = {}
    if so_far is not None:
        in_specs.append(pl.BlockSpec(memory_space=pl.ANY))
        operands.append(so_far)
        aliases = {len(operands) - 1: 0}
    return pl.pallas_call(
        debias_body,
        grid_spec=pltpu.PrefetchScalarGridSpec(
            num_scalar_prefetch=1,
            grid=(same.shape[0], split),
            in_specs=in_specs,
            out_specs=pl.BlockSpec((2 * rows, width), wide),
        ),
        out_shape=jax.ShapeDtypeStruct(p.shape, F32),
        input_output_aliases=aliases,
        name="debias",
    )(*operands)


def shards(params, weights):
    p = params[0]
    node_count = lax.axis_size(NODE)
    nodes = lax.axis_size(RING)
    blocks = lax.axis_size(BLOCKS)
    rows_all, hidden = p.shape
    rows = rows_all // nodes
    cols = hidden // 2
    width = hidden // blocks

    def moved(value, where):
        return lax.ppermute(value, NODE, [(i, where(i) % node_count) for i in range(node_count)])

    near = moved(p, lambda i: i + 1 if i % 2 == 0 else i + nodes - 1)
    weight = jnp.broadcast_to(weights.astype(p.dtype)[0], (rows_all, LANES))
    chunks = [jnp.concatenate([p[:, :cols], weight], axis=1), p[:, cols:]]
    own = [to_all(chunk.reshape(nodes, rows, -1), RING) for chunk in chunks]
    prev = [moved(piece[1:], lambda i: i + nodes) for piece in own]

    pieces = to_all(block_sums(own[0], own[1], width, blocks), BLOCKS)
    summed = jnp.sum(pieces, axis=0)
    mean = summed[:, :width] / summed[:, width : width + 1]
    means = to_all(jnp.broadcast_to(mean[None], (blocks, rows, width)), BLOCKS)
    mine = mean.reshape(rows, nodes, width // nodes).swapaxes(0, 1)
    average = to_all(mine, RING).reshape(rows_all, width // nodes)

    at = lax.axis_index(RING).astype(jnp.int32).reshape(1)
    debiased = None
    for k in range(2):
        totals = chip_sums(own[k], prev[k], own[0], prev[0], cols)
        same = to_all(totals, "y")
        swap = lax.ppermute(same, "core", [(0, 1), (1, 0)])
        debiased = debias(at, p, near, same, swap, own[0], prev[0], k, cols, debiased)

    parts = sum(
        deviations(own[k], prev[k], own[0], prev[0], means, k * blocks // 2, cols) for k in range(2)
    )
    parts = jnp.sum(parts, axis=(1, 2))
    splits = lax.axis_size("blk")
    sent = jnp.broadcast_to(parts[:, None], (nodes, splits)).reshape(nodes * splits, 1)
    spread = jnp.sum(to_all(sent, (*RING, "blk")), axis=0) / (rows_all * splits * hidden)
    return debiased[None], average, spread


def solution(mesh):
    finer = Mesh(
        mesh.devices.reshape(2, 8, 4, 2, mesh.shape["blk"]),
        (*NODE, "blk"),
    )
    return jax.shard_map(
        shards,
        mesh=finer,
        in_specs=(P(NODE, "blk", None), P(NODE)),
        out_specs=(P(NODE, "blk", None), P("blk", NODE), P(NODE)),
        check_vma=False,
    )
```

```python
import jax
import jax.numpy as jnp
from jax import lax
from jax.experimental import pallas as pl
from jax.experimental.pallas import tpu as pltpu
from jax.sharding import Mesh
from jax.sharding import PartitionSpec as P

NODE = ("xl", "z", "y", "core")
RING = ("y", "core")
BLOCKS = ("xl", "z")
CHUNKS = 2
LANES = 128
F32 = jnp.float32


def to_all(value, axes):
    return lax.all_to_all(value, axes, 0, 0, tiled=True)


def columns(ref):
    return [ref[k].astype(F32) for k in range(ref.shape[0])]


def block_sums_body(a_ref, b_ref, w_ref, out_ref):
    w = columns(w_ref)
    total = sum(w[1:], w[0])
    first_half = pl.program_id(0) < pl.num_programs(0) // 2
    for ref, chosen in ((a_ref, first_half), (b_ref, jnp.logical_not(first_half))):
        pl.when(chosen)(lambda ref=ref: fill_sums(ref, w, total, out_ref))


def fill_sums(own_ref, w, total, out_ref):
    pieces, _, wide = out_ref.shape
    width = wide - LANES
    for q in range(pieces):
        for t in range(width // LANES):
            at = slice(q * width + t * LANES, q * width + (t + 1) * LANES)
            acc = w[0] * own_ref[0, :, at].astype(F32)
            for k in range(1, len(w)):
                acc = acc + w[k] * own_ref[k, :, at].astype(F32)
            out_ref[q, :, t * LANES : (t + 1) * LANES] = acc
        out_ref[q, :, width:] = total


def spare(ref_array, cols):
    return pl.BlockSpec((*ref_array.shape[:2], LANES), lambda *_: (0, 0, cols // LANES))


def block_sums(own, width, blocks):
    nodes, rows, cols = own[1].shape
    pieces = 4
    half = blocks // pieces // 2
    block = (nodes, rows, pieces * width)
    return pl.pallas_call(
        block_sums_body,
        grid=(2 * half,),
        in_specs=[
            pl.BlockSpec(block, lambda s: (0, 0, jnp.minimum(s, half - 1))),
            pl.BlockSpec(block, lambda s: (0, 0, jnp.maximum(s - half, 0))),
            spare(own[0], cols),
        ],
        out_specs=pl.BlockSpec((pieces, rows, width + LANES), lambda s: (s, 0, 0)),
        out_shape=jax.ShapeDtypeStruct((blocks, rows, width + LANES), F32),
        name="block_sums",
    )(own[0], own[1], own[0])


def chip_sums_body(own_ref, prev_ref, w_ref, v_ref, out_ref):
    w, v = columns(w_ref), columns(v_ref)
    chips, _, width = out_ref.shape
    for t in range(width // LANES):
        at = slice(t * LANES, (t + 1) * LANES)
        after = [None] * chips
        for y in range(chips - 1, 0, -1):
            k = 2 * y
            pair = v[k - 1] * prev_ref[k - 1, :, at].astype(F32)
            pair = pair + v[k] * prev_ref[k, :, at].astype(F32)
            after[y - 1] = pair if after[y] is None else after[y] + pair
        before = None
        for y in range(chips):
            parts = [part for part in (before, after[y]) if part is not None]
            out_ref[y, :, at] = sum(parts[1:], parts[0])
            if y < chips - 1:
                k = 2 * y
                pair = w[k] * own_ref[k, :, at].astype(F32)
                pair = pair + w[k + 1] * own_ref[k + 1, :, at].astype(F32)
                before = pair if before is None else before + pair


def chip_sums(own, prev, own0, prev0, cols):
    nodes, rows = own.shape[:2]
    steps = 4
    width = cols // steps
    return pl.pallas_call(
        chip_sums_body,
        grid=(steps,),
        in_specs=[
            pl.BlockSpec((nodes, rows, width), lambda s: (0, 0, s)),
            pl.BlockSpec((nodes - 1, rows, width), lambda s: (0, 0, s)),
            spare(own0, cols),
            spare(prev0, cols),
        ],
        out_specs=pl.BlockSpec((nodes // 2, rows, width), lambda s: (0, 0, s)),
        out_shape=jax.ShapeDtypeStruct((nodes // 2, rows, cols), F32),
        name="chip_sums",
    )(own, prev, own0, prev0)


def deviations_body(*refs):
    own_refs, prev_refs = refs[:CHUNKS], refs[CHUNKS : 2 * CHUNKS]
    w_ref, v_ref, means_ref, out_ref = refs[2 * CHUNKS :]
    w, v = columns(w_ref), columns(v_ref)
    nodes = len(w)
    pieces, _, width = means_ref.shape
    inverse = []
    for c in range(nodes):
        terms = w[: c + 1] + v[c:]
        inverse.append(1.0 / sum(terms[1:], terms[0]))
    step = pl.program_id(0)

    @pl.when(step == 0)
    def _():
        out_ref[...] = jnp.zeros(out_ref.shape, F32)

    def fill(own_ref, prev_ref):
        accs = [out_ref[c] for c in range(nodes)]
        for q in range(pieces):
            for t in range(width // LANES):
                at = slice(q * width + t * LANES, q * width + (t + 1) * LANES)
                mean = means_ref[q, :, t * LANES : (t + 1) * LANES]
                after = [None] * nodes
                for c in range(nodes - 1, 0, -1):
                    term = v[c - 1] * prev_ref[c - 1, :, at].astype(F32)
                    after[c - 1] = term if after[c] is None else after[c] + term
                before = None
                for c in range(nodes):
                    term = w[c] * own_ref[c, :, at].astype(F32)
                    before = term if before is None else before + term
                    value = before if after[c] is None else before + after[c]
                    gap = value * inverse[c] - mean
                    accs[c] = accs[c] + gap * gap
        for c in range(nodes):
            out_ref[c] = accs[c]

    per = pl.num_programs(0) // CHUNKS
    for q in range(CHUNKS):
        pl.when(step // per == q)(lambda q=q: fill(own_refs[q], prev_refs[q]))


def deviations(own, prev, means, cols):
    nodes, rows = own[0].shape[:2]
    blocks, _, piece = means.shape
    pieces = 4
    steps = blocks // pieces
    per = steps // CHUNKS
    width = pieces * piece

    def near(count, q):
        return pl.BlockSpec((count, rows, width), lambda s: (0, 0, jnp.clip(s - q * per, 0, per - 1)))

    return pl.pallas_call(
        deviations_body,
        grid=(steps,),
        in_specs=[
            *[near(nodes, q) for q in range(CHUNKS)],
            *[near(nodes - 1, q) for q in range(CHUNKS)],
            spare(own[0], cols),
            spare(prev[0], cols),
            pl.BlockSpec((pieces, rows, piece), lambda s: (s, 0, 0)),
        ],
        out_specs=pl.BlockSpec((nodes, rows, LANES), lambda s: (0, 0, 0)),
        out_shape=jax.ShapeDtypeStruct((nodes, rows, LANES), F32),
        name="deviations",
    )(*own, *prev, own[0], prev[0], means)


def debias_body(at_ref, p_ref, near_ref, same_ref, swap_ref, w_ref, v_ref, *rest):
    out_ref = rest[-1]
    c = at_ref[0]
    even = c % 2 == 0
    rows = w_ref.shape[1]
    w = [value[:, 0:1] for value in columns(w_ref)]
    v = [None] + [value[:, 0:1] for value in columns(v_ref)]
    scale = own = other = w[0]
    for k in range(1, len(w)):
        scale = scale + jnp.where(k <= c, w[k], v[k])
        own = jnp.where(k == c, w[k], own)
        if k % 2:
            other = jnp.where(k == c + 1, v[k], other)
        else:
            other = jnp.where(k == c - 1, w[k], other)
    inverse = 1.0 / scale
    own, other = own * inverse, other * inverse
    same, swap = same_ref[0] * inverse, swap_ref[0] * inverse
    halves = (jnp.where(even, same, swap), jnp.where(even, swap, same))
    for half, total in enumerate(halves):
        at = slice(half * rows, (half + 1) * rows)
        out_ref[at] = total + own * p_ref[at].astype(F32) + other * near_ref[at].astype(F32)


def debias(at, p, near, same, swap, own0, prev0, chunk, so_far):
    chips, rows, cols = same.shape
    wide = pl.BlockSpec((2 * rows, cols), lambda y, at: (y, chunk))
    part = pl.BlockSpec((1, rows, cols), lambda y, at: (y, 0, 0))
    in_specs = [wide, wide, part, part, spare(own0, cols), spare(prev0, cols)]
    operands = [at, p, near, same, swap, own0, prev0]
    aliases = {}
    if so_far is not None:
        in_specs.append(pl.BlockSpec(memory_space=pl.ANY))
        operands.append(so_far)
        aliases = {len(operands) - 1: 0}
    return pl.pallas_call(
        debias_body,
        grid_spec=pltpu.PrefetchScalarGridSpec(
            num_scalar_prefetch=1,
            grid=(chips,),
            in_specs=in_specs,
            out_specs=wide,
        ),
        out_shape=jax.ShapeDtypeStruct(p.shape, F32),
        input_output_aliases=aliases,
        name="debias",
    )(*operands)


def body(params, weights):
    p = params[0]
    node_count = lax.axis_size(NODE)
    nodes = lax.axis_size(RING)
    blocks = lax.axis_size(BLOCKS)
    splits = lax.axis_size("blk")
    rows_all, hidden = p.shape
    rows = rows_all // nodes
    cols = hidden // CHUNKS
    width = hidden // blocks
    piece = width // nodes

    def moved(value, where):
        return lax.ppermute(value, NODE, [(i, where(i) % node_count) for i in range(node_count)])

    near = moved(p, lambda i: i + 1 if i % 2 == 0 else i + nodes - 1)
    weight = jnp.broadcast_to(weights.astype(p.dtype)[0], (rows_all, LANES))
    chunks = [jnp.concatenate([p[:, :cols], weight], axis=1), p[:, cols:]]
    own, prev = [], []
    for k in range(CHUNKS):
        own.append(to_all(chunks[k].reshape(nodes, rows, -1), RING))
        prev.append(moved(own[k][1:], lambda i: i + nodes))

    summed = jnp.sum(to_all(block_sums(own, width, blocks), BLOCKS), axis=0)
    mean = summed[:, :width] / summed[:, width : width + 1]
    means = to_all(jnp.broadcast_to(mean[None], (blocks, rows, width)), BLOCKS)

    at = lax.axis_index(RING).astype(jnp.int32).reshape(1)
    debiased = None
    for k in range(CHUNKS):
        totals = chip_sums(own[k], prev[k], own[0], prev[0], cols)
        same = to_all(totals, "y")
        swap = lax.ppermute(same, "core", [(0, 1), (1, 0)])
        debiased = debias(at, p, near, same, swap, own[0], prev[0], k, debiased)

    parts = jnp.sum(deviations(own, prev, means, cols), axis=(1, 2))
    mine = mean.reshape(rows, nodes, piece).swapaxes(0, 1)
    sent = jnp.concatenate(
        [mine, jnp.broadcast_to(parts[:, None, None], (nodes, rows, LANES - piece))], axis=2
    )
    sent = jnp.broadcast_to(sent[:, None], (nodes, splits, rows, LANES))
    got = to_all(sent.reshape(nodes * splits, rows, LANES), (*RING, "blk"))
    spread = jnp.sum(got[:, 0, piece : piece + 1], axis=0) / (rows_all * splits * hidden)
    got = got.reshape(nodes, splits, rows, LANES)
    average = lax.dynamic_index_in_dim(got, lax.axis_index("blk"), 1, keepdims=False)
    average = average[:, :, :piece].reshape(rows_all, piece)
    return debiased[None], average, spread


def solution(mesh):
    finer = Mesh(
        mesh.devices.reshape(2, 8, 4, 2, mesh.shape["blk"]),
        (*NODE, "blk"),
    )
    return jax.shard_map(
        body,
        mesh=finer,
        in_specs=(P(NODE, "blk", None), P(NODE)),
        out_specs=(P(NODE, "blk", None), P("blk", NODE), P(NODE)),
        check_vma=False,
    )
```

```python
import jax
import jax.numpy as jnp
from jax import lax
from jax.experimental import pallas as pl
from jax.experimental.pallas import tpu as pltpu
from jax.sharding import Mesh
from jax.sharding import PartitionSpec as P

NODE = ("xl", "z", "y", "core")
RING = ("y", "core")
BLOCKS = ("xl", "z")
CHUNKS = 2
LANES = 128
F32 = jnp.float32


def to_all(value, axes):
    return lax.all_to_all(value, axes, 0, 0, tiled=True)


def columns(ref):
    return [ref[k].astype(F32) for k in range(ref.shape[0])]


def block_sums_body(own_ref, w_ref, out_ref):
    pieces, _, wide = out_ref.shape
    width = wide - LANES
    w = columns(w_ref)
    total = sum(w[1:], w[0])
    for q in range(pieces):
        for t in range(width // LANES):
            at = slice(q * width + t * LANES, q * width + (t + 1) * LANES)
            acc = w[0] * own_ref[0, :, at].astype(F32)
            for k in range(1, len(w)):
                acc = acc + w[k] * own_ref[k, :, at].astype(F32)
            out_ref[q, :, t * LANES : (t + 1) * LANES] = acc
        out_ref[q, :, width:] = total


def whole(array):
    return pl.BlockSpec(array.shape, lambda *_: (0,) * array.ndim)


def block_sums(own, w, width, blocks):
    nodes, rows, _ = own.shape
    pieces = 4
    return pl.pallas_call(
        block_sums_body,
        grid=(blocks // pieces,),
        in_specs=[pl.BlockSpec((nodes, rows, pieces * width), lambda s: (0, 0, s)), whole(w)],
        out_specs=pl.BlockSpec((pieces, rows, width + LANES), lambda s: (s, 0, 0)),
        out_shape=jax.ShapeDtypeStruct((blocks, rows, width + LANES), F32),
        name="block_sums",
    )(own, w)


def chip_sums_body(at_ref, own_ref, prev_ref, w_ref, v_ref, *out_refs):
    w, v = columns(w_ref), columns(v_ref)
    chips = len(out_refs)
    width = out_refs[0].shape[1]
    here = at_ref[0] // 2
    for t in range(width // LANES):
        at = slice(t * LANES, (t + 1) * LANES)
        after = [None] * chips
        for y in range(chips - 1, 0, -1):
            k = 2 * y
            pair = v[k] * prev_ref[k - 1, :, at].astype(F32)
            pair = pair + v[k + 1] * prev_ref[k, :, at].astype(F32)
            after[y - 1] = pair if after[y] is None else after[y] + pair
        before, sums = None, []
        for y in range(chips):
            parts = [part for part in (before, after[y]) if part is not None]
            sums.append(sum(parts[1:], parts[0]))
            if y < chips - 1:
                k = 2 * y
                pair = w[k] * own_ref[k, :, at].astype(F32)
                pair = pair + w[k + 1] * own_ref[k + 1, :, at].astype(F32)
                before = pair if before is None else before + pair
        for k in range(chips):
            chosen = sums[k]
            for y in range(1, chips):
                chosen = jnp.where(here == y, sums[y ^ k], chosen)
            out_refs[k][:, at] = chosen


def chip_sums(at, own, prev, w, v, chunk):
    nodes, rows = own.shape[:2]
    cols = prev.shape[2]
    steps = 4
    width = cols // steps
    chips = nodes // 2
    return pl.pallas_call(
        chip_sums_body,
        grid_spec=pltpu.PrefetchScalarGridSpec(
            num_scalar_prefetch=1,
            grid=(steps,),
            in_specs=[
                pl.BlockSpec((nodes, rows, width), lambda s, at: (0, 0, chunk * steps + s)),
                pl.BlockSpec((nodes - 1, rows, width), lambda s, at: (0, 0, s)),
                whole(w),
                whole(v),
            ],
            out_specs=[pl.BlockSpec((rows, width), lambda s, at: (0, s))] * chips,
        ),
        out_shape=[jax.ShapeDtypeStruct((rows, cols), F32)] * chips,
        name="chip_sums",
    )(at, own, prev, w, v)


def deviations_body(*refs):
    own_ref, prev_refs = refs[0], refs[1 : 1 + CHUNKS]
    w_ref, v_ref, means_ref, out_ref = refs[1 + CHUNKS :]
    w, v = columns(w_ref), columns(v_ref)
    nodes = len(w)
    pieces, _, width = means_ref.shape
    inverse = []
    for c in range(nodes):
        terms = w[: c + 1] + v[c + 1 :]
        inverse.append(1.0 / sum(terms[1:], terms[0]))
    step = pl.program_id(0)

    @pl.when(step == 0)
    def _():
        out_ref[...] = jnp.zeros(out_ref.shape, F32)

    def fill(prev_ref):
        accs = [out_ref[c] for c in range(nodes)]
        for q in range(pieces):
            for t in range(width // LANES):
                at = slice(q * width + t * LANES, q * width + (t + 1) * LANES)
                mean = means_ref[q, :, t * LANES : (t + 1) * LANES]
                after = [None] * nodes
                for c in range(nodes - 1, 0, -1):
                    term = v[c] * prev_ref[c - 1, :, at].astype(F32)
                    after[c - 1] = term if after[c] is None else after[c] + term
                before = None
                for c in range(nodes):
                    term = w[c] * own_ref[c, :, at].astype(F32)
                    before = term if before is None else before + term
                    value = before if after[c] is None else before + after[c]
                    gap = value * inverse[c] - mean
                    accs[c] = accs[c] + gap * gap
        for c in range(nodes):
            out_ref[c] = accs[c]

    per = pl.num_programs(0) // CHUNKS
    for q in range(CHUNKS):
        pl.when(step // per == q)(lambda q=q: fill(prev_refs[q]))


def deviations(own, prev, w, v, means):
    nodes, rows, _ = own.shape
    blocks, _, piece = means.shape
    pieces = 4
    steps = blocks // pieces
    per = steps // CHUNKS
    width = pieces * piece

    def near(q):
        return pl.BlockSpec(
            (nodes - 1, rows, width), lambda s: (0, 0, jnp.clip(s - q * per, 0, per - 1))
        )

    return pl.pallas_call(
        deviations_body,
        grid=(steps,),
        in_specs=[
            pl.BlockSpec((nodes, rows, width), lambda s: (0, 0, s)),
            *[near(q) for q in range(CHUNKS)],
            whole(w),
            whole(v),
            pl.BlockSpec((pieces, rows, piece), lambda s: (s, 0, 0)),
        ],
        out_specs=pl.BlockSpec((nodes, rows, LANES), lambda s: (0, 0, 0)),
        out_shape=jax.ShapeDtypeStruct((nodes, rows, LANES), F32),
        name="deviations",
    )(own, *prev, w, v, means)


def debias_body(at_ref, p_ref, near_ref, *refs):
    chips = (len(refs) - 3) // 2
    same_refs, swap_refs = refs[:chips], refs[chips : 2 * chips]
    w_ref, v_ref = refs[2 * chips : 2 * chips + 2]
    out_ref = refs[-1]
    c = at_ref[0]
    even = c % 2 == 0
    rows = w_ref.shape[1]
    w, v = ([value[:, 0:1] for value in columns(ref)] for ref in (w_ref, v_ref))
    scale = own = other = w[0]
    for k in range(1, len(w)):
        scale = scale + jnp.where(k <= c, w[k], v[k])
        own = jnp.where(k == c, w[k], own)
        if k % 2:
            other = jnp.where(k == c + 1, v[k], other)
        else:
            other = jnp.where(k == c - 1, w[k], other)
    inverse = 1.0 / scale
    own, other = own * inverse, other * inverse
    for k in range(chips):
        at = pl.ds(pl.multiple_of(2 * rows * ((c // 2) ^ k), 2 * rows), 2 * rows)
        same, swap = same_refs[k][...] * inverse, swap_refs[k][...] * inverse
        halves = (jnp.where(even, same, swap), jnp.where(even, swap, same))
        p, near = p_ref[at].astype(F32), near_ref[at].astype(F32)
        parts = [
            total + own * p[h * rows : (h + 1) * rows] + other * near[h * rows : (h + 1) * rows]
            for h, total in enumerate(halves)
        ]
        out_ref[at] = jnp.concatenate(parts, axis=0)


def debias(at, p, near, same, swap, w, v, chunk, so_far):
    rows, cols = same[0].shape
    steps = 4
    width = cols // steps
    wide = pl.BlockSpec((p.shape[0], width), lambda s, at: (0, chunk * steps + s))
    part = pl.BlockSpec((rows, width), lambda s, at: (0, s))
    in_specs = [wide, wide, *[part] * (len(same) + len(swap)), whole(w), whole(v)]
    operands = [at, p, near, *same, *swap, w, v]
    body = debias_body
    aliases = {}
    if so_far is not None:
        in_specs.append(pl.BlockSpec(memory_space=pl.ANY))
        operands.append(so_far)
        aliases = {len(operands) - 1: 0}
        body = lambda *refs: debias_body(*refs[:-2], refs[-1])
    return pl.pallas_call(
        body,
        grid_spec=pltpu.PrefetchScalarGridSpec(
            num_scalar_prefetch=1,
            grid=(steps,),
            in_specs=in_specs,
            out_specs=wide,
        ),
        out_shape=jax.ShapeDtypeStruct(p.shape, F32),
        input_output_aliases=aliases,
        name="debias",
    )(*operands)


def body(params, weights):
    p = params[0]
    node_count = lax.axis_size(NODE)
    nodes = lax.axis_size(RING)
    blocks = lax.axis_size(BLOCKS)
    splits = lax.axis_size("blk")
    rows_all, hidden = p.shape
    rows = rows_all // nodes
    cols = hidden // CHUNKS
    width = hidden // blocks
    piece = width // nodes

    def moved(value, where):
        return lax.ppermute(value, NODE, [(i, where(i) % node_count) for i in range(node_count)])

    near = moved(p, lambda i: i + 1 if i % 2 == 0 else i + nodes - 1)
    own = to_all(p.reshape(nodes, rows, hidden), RING)
    at = lax.axis_index(RING).astype(jnp.int32)
    place = jnp.arange(nodes)[:, None, None] == at
    w = jnp.where(place, weights.astype(F32)[0], 0.0)
    w = jnp.broadcast_to(w, (nodes, rows, LANES))
    for step in (1, 2, 4):
        w = w + moved(w, lambda i, step=step: i ^ step)
    v = moved(w, lambda i: i + nodes)
    at = at.reshape(1)
    prev = []
    for k in range(CHUNKS):
        prev.append(moved(own[1:, :, k * cols : (k + 1) * cols], lambda i: i + nodes))

    summed = jnp.sum(to_all(block_sums(own, w, width, blocks), BLOCKS), axis=0)
    mean = summed[:, :width] / summed[:, width : width + 1]
    means = to_all(jnp.broadcast_to(mean[None], (blocks, rows, width)), BLOCKS)

    debiased = None
    for k in range(CHUNKS):
        same = list(chip_sums(at, own, prev[k], w, v, k))
        for step in range(1, len(same)):
            same[step] = moved(same[step], lambda i, step=step: i ^ (2 * step))
        swap = [moved(value, lambda i: i ^ 1) for value in same]
        debiased = debias(at, p, near, same, swap, w, v, k, debiased)

    parts = jnp.sum(deviations(own, prev, w, v, means), axis=(1, 2))
    mine = mean.reshape(rows, nodes, piece).swapaxes(0, 1)
    sent = jnp.concatenate(
        [mine, jnp.broadcast_to(parts[:, None, None], (nodes, rows, LANES - piece))], axis=2
    )
    sent = jnp.broadcast_to(sent[:, None], (nodes, splits, rows, LANES))
    got = to_all(sent.reshape(nodes * splits, rows, LANES), (*RING, "blk"))
    spread = jnp.sum(got[:, 0, piece : piece + 1], axis=0) / (rows_all * splits * hidden)
    got = got.reshape(nodes, splits, rows, LANES)
    average = lax.dynamic_index_in_dim(got, lax.axis_index("blk"), 1, keepdims=False)
    average = average[:, :, :piece].reshape(rows_all, piece)
    return debiased[None], average, spread


def solution(mesh):
    finer = Mesh(
        mesh.devices.reshape(2, 8, 4, 2, mesh.shape["blk"]),
        (*NODE, "blk"),
    )
    return jax.shard_map(
        body,
        mesh=finer,
        in_specs=(P(NODE, "blk", None), P(NODE)),
        out_specs=(P(NODE, "blk", None), P("blk", NODE), P(NODE)),
        check_vma=False,
    )
```
